32 devices in a mesh: dp: 4 (over y, core), fsdp: 8 (over z, x).
Axes of the slice: x: 2, y: 2, z: 4, core: 2. Of those that a mesh axis runs over, the one named last changes fastest.
Arguments:
- tokens: bfloat16 [27648, 768], P(('dp', 'fsdp')), may hold values from -6 to 6
- segment_ids: int32 [27648], P(('dp', 'fsdp')), may hold values from 0 to 191, never falling along the last dimension, each value on 1 to 288 neighbouring positions
- position_ids: int32 [27648], P(('dp', 'fsdp')), may hold values from 0 to 287, as said below
- cotangent: bfloat16 [27648, 768], P(('dp', 'fsdp')), may hold values from -6 to 6
- query_weight: bfloat16 [768, 768], P(('dp', 'fsdp')), may hold values from -0.21875 to 0.21875
- key_weight: bfloat16 [768, 768], P(('dp', 'fsdp')), may hold values from -0.21875 to 0.21875
- value_weight: bfloat16 [768, 768], P(('dp', 'fsdp')), may hold values from -0.21875 to 0.21875
- out_weight: bfloat16 [768, 768], P(('dp', 'fsdp')), may hold values from -0.875 to 0.875
- up_weight: bfloat16 [768, 3072], P(('dp', 'fsdp')), may hold values from -0.21875 to 0.21875
- down_weight: bfloat16 [3072, 768], P(('dp', 'fsdp')), may hold values from -0.109375 to 0.109375
- query_bias: bfloat16 [768], P(('dp', 'fsdp')), may hold values from -3 to 3
- value_bias: bfloat16 [768], P(('dp', 'fsdp')), may hold values from -3 to 3
- out_bias: bfloat16 [768], P(('dp', 'fsdp')), may hold values from -3 to 3
- up_bias: bfloat16 [3072], P(('dp', 'fsdp')), may hold values from -3 to 3
- down_bias: bfloat16 [768], P(('dp', 'fsdp')), may hold values from -3 to 3
- first_gain: bfloat16 [768], P(('dp', 'fsdp')), may hold values from 0.099609375 to 1.8984375
- first_shift: bfloat16 [768], P(('dp', 'fsdp')), may hold values from -3 to 3
- second_gain: bfloat16 [768], P(('dp', 'fsdp')), may hold values from 0.099609375 to 1.8984375
- second_shift: bfloat16 [768], P(('dp', 'fsdp')), may hold values from -3 to 3
Outputs:
- block_out: bfloat16 [27648, 768], P(('dp', 'fsdp'))
- token_grad: float32 [27648, 768], P(('dp', 'fsdp'))
- query_weight_grad: float32 [768, 768], P(('dp', 'fsdp'))
- key_weight_grad: float32 [768, 768], P(('dp', 'fsdp'))
- value_weight_grad: float32 [768, 768], P(('dp', 'fsdp'))
- out_weight_grad: float32 [768, 768], P(('dp', 'fsdp'))
- up_weight_grad: float32 [768, 3072], P(('dp', 'fsdp'))
- down_weight_grad: float32 [3072, 768], P(('dp', 'fsdp'))
- query_bias_grad: float32 [768], P(('dp', 'fsdp'))
- value_bias_grad: float32 [768], P(('dp', 'fsdp'))
- out_bias_grad: float32 [768], P(('dp', 'fsdp'))
- up_bias_grad: float32 [3072], P(('dp', 'fsdp'))
- down_bias_grad: float32 [768], P(('dp', 'fsdp'))
- first_gain_grad: float32 [768], P(('dp', 'fsdp'))
- first_shift_grad: float32 [768], P(('dp', 'fsdp'))
- second_gain_grad: float32 [768], P(('dp', 'fsdp'))
- second_shift_grad: float32 [768], P(('dp', 'fsdp'))
The draws below stay inside these ranges and needn't reach their ends.
Inputs may be any that keep to these rules, and one draw needn't show every extreme that they name: `position_ids`: positions count up by one along the rows; they are 0 at the first row of each sequence of 288 rows and at some other rows; the first sequence has no restart after its first row.
All inputs are finite; a program needn't handle non-finite values.
Results may differ from the reference program's by a relative error of at most 0.013.
Values may be sent and summed in bfloat16 or wider, within the bound.
A program may use at most 192 MiB of HBM per device.

```python
import math
import jax
import jax.numpy as jnp
import numpy as np
from jax import lax

D = 768
HEADS = 12
HEAD_DIM = 64
FF = 3072
LEN = 288
SEQ_DEV = 3
TOKENS = 27648


def draw_position_ids(key, part):
    indices = jnp.arange(TOKENS, dtype=jnp.int32)
    coin_flips = jax.random.randint(key, (TOKENS,), 0, 40)
    random_starts = jnp.logical_and(coin_flips == 0, indices >= LEN)
    restarts = jnp.logical_or(indices % LEN == 0, random_starts)
    marked = jnp.where(restarts, indices, 0)
    latest_start = lax.cummax(marked, axis=0)
    return (indices - latest_start).astype(jnp.int32)


def block_levels(rng, dims, pieces, low, high):
    gain, own = 1.0, jax.random.fold_in(rng, 6)
    for dim, blocks in pieces:
        heights = jnp.exp(jax.random.uniform(jax.random.fold_in(own, dim), (blocks,), jnp.float32, low / len(pieces), high / len(pieces)))
        gain = gain * jnp.repeat(heights, dims[dim] // blocks).reshape([-1 if axis == dim else 1 for axis in range(len(dims))])
    return gain


def split_up(number_of, total, reach, skew):
    loads = [(1 << 20) // math.isqrt(standing ** skew) + 1 for standing in range(2, number_of + 1)]
    surplus, holding = total - reach - (number_of - 1), [1] * (number_of - 1)
    while surplus > 0:
        candidates = [i for i in range(number_of - 1) if holding[i] < reach]
        mass, budget = sum([loads[i] for i in candidates]), surplus
        for i in candidates:
            more = min(reach - holding[i], max(1, budget * loads[i] // mass), surplus)
            holding[i] = holding[i] + more
            surplus = surplus - more
    return np.array([reach] + holding)


def uneven_parts(rng, amount, total, limit, lean):
    if amount == 2:
        one = jax.random.randint(rng, (), max(1, total - limit), min(limit, total - 1) + 1)
        return jnp.stack([one, total - one])
    tallies = jnp.asarray(split_up(amount, total, limit, lean), jnp.int32)
    pairs = (amount - 1) // 2
    donor, sink = tallies[1:1 + 2 * pairs:2], tallies[2:2 + 2 * pairs:2]
    slack = jnp.minimum(donor - 1, limit - sink)
    shifted = jax.random.randint(jax.random.fold_in(rng, 1), (pairs,), 0, 1 << 20) % (slack + 1)
    tallies = tallies.at[1:1 + 2 * pairs:2].set(donor - shifted).at[2:2 + 2 * pairs:2].set(sink + shifted)
    return tallies[jax.random.permutation(jax.random.fold_in(rng, 2), amount)]


def noise(rng, dims, width, reach, split=(), held_as=jnp.bfloat16):
    values = width * jax.random.normal(rng, dims, jnp.float32)
    if split:
        values = values * block_levels(rng, dims, split, -0.22, 0.18)
    return jnp.clip(values, -reach, reach).astype(held_as)


def setup_inputs(seed: int = 0) -> dict:
    key_of = jax.random.split(jax.random.key(seed), 20)
    return {
        "tokens": noise(key_of[0], (TOKENS, D), 1.0, 6.0, ((0, 32),)),
        "segment_ids": jnp.searchsorted(jnp.cumsum(uneven_parts(key_of[1], TOKENS * 2 // LEN, TOKENS, LEN, 0)), jnp.arange(TOKENS), side="right").astype(jnp.int32),
        "position_ids": draw_position_ids(jax.random.fold_in(key_of[19], 71), 0),
        "cotangent": noise(key_of[3], (TOKENS, D), 1.0, 6.0, ((0, 32),)),
        "query_weight": noise(key_of[4], (D, D), D ** -0.5, 0.21875, ((0, 32),)),
        "key_weight": noise(key_of[5], (D, D), D ** -0.5, 0.21875, ((0, 32),)),
        "value_weight": noise(key_of[6], (D, D), D ** -0.5, 0.21875, ((0, 32),)),
        "out_weight": noise(key_of[7], (D, D), (D // 16) ** -0.5, 0.875, ((0, 32),)),
        "up_weight": noise(key_of[8], (D, FF), D ** -0.5, 0.21875, ((0, 32),)),
        "down_weight": noise(key_of[9], (FF, D), FF ** -0.5, 0.109375, ((0, 32),)),
        "query_bias": noise(key_of[10], (D,), 0.5, 3.0, ((0, 32),)),
        "value_bias": noise(key_of[11], (D,), 0.5, 3.0, ((0, 32),)),
        "out_bias": noise(key_of[12], (D,), 0.5, 3.0, ((0, 32),)),
        "up_bias": noise(key_of[13], (FF,), 0.5, 3.0, ((0, 32),)),
        "down_bias": noise(key_of[14], (D,), 0.5, 3.0, ((0, 32),)),
        "first_gain": jnp.clip(1.0 + 0.18 * jax.random.normal(key_of[15], (D,), jnp.float32), 0.099609375, 1.8984375).astype(jnp.bfloat16),
        "first_shift": noise(key_of[16], (D,), 0.5, 3.0, ((0, 32),)),
        "second_gain": jnp.clip(1.0 + 0.18 * jax.random.normal(key_of[17], (D,), jnp.float32), 0.099609375, 1.8984375).astype(jnp.bfloat16),
        "second_shift": noise(key_of[18], (D,), 0.5, 3.0, ((0, 32),)),
    }


@jax.custom_vjp
def low(v):
    return lax.optimization_barrier(v.astype(jnp.bfloat16)).astype(jnp.float32)

@jax.custom_vjp
def low_back(v):
    return v

def low_keep(v):
    return (low(v), None)

def low_pass(kept, grad):
    return (grad,)

def back_keep(v):
    return (v, None)

def back_low(kept, grad):
    return (low(grad),)
low.defvjp(low_keep, low_pass)
low_back.defvjp(back_keep, back_low)
EPSILON = 1e-06
NEGATIVE = -1000000000.0
HALF_ROOT = 0.7071067811865476
PRECISE = lax.Precision.HIGHEST

def layer_norm(values, scales, shifts):
    centre = lax.optimization_barrier(jnp.mean(values, axis=-1, keepdims=True))
    centred = values - centre
    spread = lax.optimization_barrier(jnp.mean(centred * centred, axis=-1, keepdims=True))
    return centred * lax.rsqrt(spread + EPSILON) * scales + shifts

def gelu_exact(values):
    return 0.5 * values * (1.0 + lax.erf(values * HALF_ROOT))

def visible(segments, positions):
    offsets = positions - jnp.arange(positions.shape[-1], dtype=jnp.int32)[None, :]
    same_segment = segments[:, :, None] == segments[:, None, :]
    same_run = offsets[:, :, None] == offsets[:, None, :]
    return jnp.logical_and(same_segment, same_run)[:, None]

def matmul(left_side, right_side):
    return jnp.dot(left_side, right_side, precision=PRECISE)

def split_heads(tensor):
    return tensor.reshape(tensor.shape[0] // LEN, LEN, HEADS, HEAD_DIM)

def forward(segments, positions, inputs, query_weight, key_weight, value_weight, out_weight, up_weight, down_weight, query_bias, value_bias, out_bias, up_bias, down_bias, first_gain, first_shift, second_gain, second_shift):
    query_vectors = low_back(low(matmul(inputs, query_weight) + query_bias))
    key_vectors = low_back(low(matmul(inputs, key_weight)))
    value_vectors = low_back(low(matmul(inputs, value_weight) + value_bias))
    allowed = visible(segments.reshape(-1, LEN), positions.reshape(-1, LEN))
    raw_scores = jnp.einsum('sqhd,skhd->shqk', split_heads(query_vectors), split_heads(key_vectors), precision=PRECISE)
    scores = jnp.where(allowed, low_back(raw_scores * 0.125), NEGATIVE)
    peak_score = lax.optimization_barrier(jnp.max(scores, axis=-1, keepdims=True))
    exponents = jnp.exp(scores - peak_score)
    attention_probs = low(exponents / lax.optimization_barrier(jnp.sum(exponents, axis=-1, keepdims=True)))
    attended = jnp.einsum('shqk,skhd->sqhd', attention_probs, split_heads(value_vectors), precision=PRECISE)
    mixed_heads = low_back(low(attended.reshape(inputs.shape)))
    branch = low_back(matmul(mixed_heads, out_weight) + out_bias)
    first_out = layer_norm(inputs + branch, first_gain, first_shift)
    hidden = low_back(matmul(low(first_out), up_weight) + up_bias)
    activated = low(gelu_exact(hidden))
    ffn_out = low_back(matmul(activated, down_weight) + down_bias)
    return layer_norm(first_out + ffn_out, second_gain, second_shift)

def reference(tokens, segment_ids, position_ids, cotangent, query_weight, key_weight, value_weight, out_weight, up_weight, down_weight, query_bias, value_bias, out_bias, up_bias, down_bias, first_gain, first_shift, second_gain, second_shift):
    params = tuple((weight_array.astype(jnp.float32) for weight_array in (query_weight, key_weight, value_weight, out_weight, up_weight, down_weight, query_bias, value_bias, out_bias, up_bias, down_bias, first_gain, first_shift, second_gain, second_shift)))
    block_rows = SEQ_DEV * LEN
    blocks = tokens.shape[0] // block_rows

    def scan_step(totals, block_items):
        token_block, segment_block, position_block, cotangent_block = block_items

        def closed(inputs, *weights):
            return forward(segment_block, position_block, inputs, *weights)
        result, pullback = jax.vjp(closed, token_block.astype(jnp.float32), *params)
        gradients = pullback(cotangent_block.astype(jnp.float32))
        return (jax.tree.map(jnp.add, totals, tuple(gradients[1:])), (result.astype(jnp.bfloat16), gradients[0]))
    initial = tuple((jnp.zeros_like(weight_array) for weight_array in params))
    totals, (outputs, token_grads) = lax.scan(scan_step, initial, (tokens.reshape(blocks, block_rows, D), segment_ids.reshape(blocks, block_rows), position_ids.reshape(blocks, block_rows), cotangent.reshape(blocks, block_rows, D)))
    return (outputs.reshape(-1, D), token_grads.reshape(-1, D), totals[0], totals[1], totals[2], totals[3], totals[4], totals[5], totals[6], totals[7], totals[8], totals[9], totals[10], totals[11], totals[12], totals[13], totals[14])
```

```python
import functools
import jax
import jax.numpy as jnp
from jax import lax
from jax.sharding import PartitionSpec as P
from jax.experimental import pallas as pl
from jax.experimental.pallas import tpu as pltpu

MESH = pl.DeviceIdType.MESH
ANY = pl.BlockSpec(memory_space=pl.ANY)
F32 = jnp.float32
BF16 = jnp.bfloat16


NAMES = ('dp', 'fsdp')


class Place:
    def __init__(self):
        dp, fs = lax.axis_index("dp"), lax.axis_index("fsdp")
        self.y, self.c = dp // 2, dp % 2
        self.z, self.x = fs // 2, fs % 2

    def device(self, ry=0, rc=0, rz=0, rx=0):
        y = 1 - self.y if ry else self.y
        c = 1 - self.c if rc else self.c
        x = 1 - self.x if rx else self.x
        return (y * 2 + c, ((self.z + rz) % 4) * 2 + x)

    def slot(self, ry=0, rc=0, rz=0, rx=0):
        y = 1 - self.y if ry else self.y
        c = 1 - self.c if rc else self.c
        x = 1 - self.x if rx else self.x
        return (y, c, (self.z + rz) % 4, x)


def greet(me):
    barrier = pltpu.get_barrier_semaphore()
    peers = [me.device(rx=1), me.device(ry=1), me.device(rc=1)]
    peers += [me.device(rz=k) for k in (1, 2, 3)]
    for peer in peers:
        pl.semaphore_signal(barrier, inc=1, device_id=peer, device_id_type=MESH)
    pl.semaphore_wait(barrier, 6)


def halves(ref, lead, which):
    r, n = ref.shape[-2:]
    if r >= 96:
        return ref.at[(*lead, pl.ds(which * (r // 2), r // 2), slice(None))]
    first = n // 256 * 128
    return ref.at[(*lead, slice(None), pl.ds(first if which else 0, n - first if which else first))]


Z, X, Y, XY, YX, C0, CX, CY, CB, CC, KINDS = 0, 3, 7, 11, 15, 19, 23, 27, 31, 35, 39


def gather_kernel(count, *refs):
    ins, outs = refs[:count], refs[count : 2 * count]
    bounce = refs[2 * count : 3 * count]
    send, recv, local = refs[3 * count :]
    me = Place()
    greet(me)
    started = []

    def remote(m, k, src, dst, **to):
        copy = pltpu.make_async_remote_copy(
            src_ref=src, dst_ref=dst, send_sem=send.at[m, k], recv_sem=recv.at[m, k],
            device_id=me.device(**to), device_id_type=MESH,
        )
        copy.start()
        started.append(copy)

    def arrived(m, k, dst):
        pltpu.make_async_remote_copy(
            src_ref=dst, dst_ref=dst, send_sem=send.at[m, k], recv_sem=recv.at[m, k],
            device_id=me.device(rc=1), device_id_type=MESH,
        ).wait_recv()

    for m in range(count):
        pltpu.make_async_copy(ins[m], bounce[m], local.at[m]).start()
    for m in range(count):
        for k in (1, 2, 3):
            remote(m, Z + k - 1, ins[m], outs[m].at[me.slot()], rz=k)
    for m in range(count):
        pltpu.make_async_copy(ins[m], bounce[m], local.at[m]).wait()
        pltpu.make_async_copy(bounce[m], outs[m].at[me.slot()], local.at[m]).start()

    def diagonal(m, j):
        slot = me.slot(rz=-j, rx=1, ry=1)
        b, c = halves(outs[m], slot, 0), halves(outs[m], slot, 1)
        arrived(m, XY + j, b)
        remote(m, CB + j, b, b, rc=1)
        arrived(m, YX + j, c)
        remote(m, CC + j, c, c, rc=1)

    def across(m, j):
        sx = me.slot(rz=-j, rx=1)
        arrived(m, X + j, outs[m].at[sx])
        b = halves(outs[m], sx, 0)
        remote(m, XY + j, b, b, ry=1)
        remote(m, CX + j, outs[m].at[sx], outs[m].at[sx], rc=1)
        sy = me.slot(rz=-j, ry=1)
        arrived(m, Y + j, outs[m].at[sy])
        c = halves(outs[m], sy, 1)
        remote(m, YX + j, c, c, rx=1)
        remote(m, CY + j, outs[m].at[sy], outs[m].at[sy], rc=1)

    def along(m, j):
        slot = me.slot(rz=-j)
        dst = outs[m].at[slot]
        src = ins[m] if j == 0 else dst
        if j:
            arrived(m, Z + j - 1, dst)
        remote(m, X + j, src, dst, rx=1)
        remote(m, Y + j, src, dst, ry=1)
        remote(m, C0 + j, src, dst, rc=1)

    for m in range(count):
        along(m, 0)
        for j in range(1, 4):
            along(m, j)
            across(m, j - 1)
        across(m, 3)
        for j in range(4):
            diagonal(m, j)
    for m in range(count):
        for j in range(4):
            arrived(m, C0 + j, outs[m].at[me.slot(rc=1, rz=-j)])
            arrived(m, CX + j, outs[m].at[me.slot(rc=1, rz=-j, rx=1)])
            arrived(m, CY + j, outs[m].at[me.slot(rc=1, rz=-j, ry=1)])
            slot = me.slot(rc=1, rz=-j, rx=1, ry=1)
            arrived(m, CB + j, halves(outs[m], slot, 0))
            arrived(m, CC + j, halves(outs[m], slot, 1))
    for copy in started:
        copy.wait_send()
    for m in range(count):
        pltpu.make_async_copy(bounce[m], outs[m].at[me.slot()], local.at[m]).wait()


def gather(arrays):
    count = len(arrays)
    return pl.pallas_call(
        functools.partial(gather_kernel, count),
        name="gather",
        out_shape=tuple(jax.ShapeDtypeStruct((2, 2, 4, 2) + a.shape, a.dtype) for a in arrays),
        in_specs=[ANY] * count,
        out_specs=(ANY,) * count,
        scratch_shapes=[pltpu.VMEM(a.shape, a.dtype) for a in arrays]
        + [
            pltpu.SemaphoreType.DMA((count, KINDS)),
            pltpu.SemaphoreType.DMA((count, KINDS)),
            pltpu.SemaphoreType.DMA((count,)),
        ],
        compiler_params=pltpu.CompilerParams(collective_id=0, has_side_effects=True),
    )(*arrays)


Q_C, Q_D, Q_X, Q_O, Q_K = 0, 16, 24, 32, 35


def scatter_kernel(count, *refs):
    ins, outs = refs[:count], refs[count : 2 * count]
    rest = refs[2 * count :]
    mine, core, diag, side, line = (rest[i * count : (i + 1) * count] for i in range(5))
    send, recv, local = rest[5 * count :]
    me = Place()
    greet(me)
    started = []

    def remote(m, k, src, dst, **to):
        copy = pltpu.make_async_remote_copy(
            src_ref=src, dst_ref=dst, send_sem=send.at[m, k], recv_sem=recv.at[m, k],
            device_id=me.device(**to), device_id_type=MESH,
        )
        copy.start()
        started.append(copy)

    def arrived(m, k, dst):
        pltpu.make_async_remote_copy(
            src_ref=dst, dst_ref=dst, send_sem=send.at[m, k], recv_sem=recv.at[m, k],
            device_id=me.device(rc=1), device_id_type=MESH,
        ).wait_recv()

    quarters = {3: dict(rx=1, ry=1), 1: dict(rx=1), 2: dict(ry=1), 0: {}}

    def load(m, q, j):
        slot = me.slot(rz=j, **quarters[q])
        return pltpu.make_async_copy(ins[m].at[slot], mine[m].at[q, j], local.at[m, q * 4 + j])

    for m in range(count):
        for q in (3, 1, 2, 0):
            for j in range(4):
                slot = me.slot(rz=j, rc=1, **quarters[q])
                remote(m, Q_C + q * 4 + j, ins[m].at[slot], core[m].at[q, j], rc=1)
                load(m, q, j).start()

    def cut(ref, which):
        return halves(ref, (), which)

    def pair(m, q, j):
        load(m, q, j).wait()
        arrived(m, Q_C + q * 4 + j, core[m].at[q, j])

    def total(dst, *parts):
        value = dst[...].astype(F32)
        for part in parts:
            value = value + part[...].astype(F32)
        dst[...] = value.astype(dst.dtype)

    def corner(m):
        for j in range(4):
            pair(m, 3, j)
            total(mine[m].at[3, j], core[m].at[3, j])
            remote(m, Q_D + j, cut(mine[m].at[3, j], 0), cut(diag[m].at[0, j], 0), ry=1)
            remote(m, Q_D + 4 + j, cut(mine[m].at[3, j], 1), cut(diag[m].at[1, j], 1), rx=1)

    def sides(m):
        for j in range(4):
            for q, to in ((1, dict(rx=1)), (2, dict(ry=1))):
                pair(m, q, j)
                arrived(m, Q_D + 4 * (q - 1) + j, cut(diag[m].at[q - 1, j], q - 1))
                for w in (0, 1):
                    parts = [cut(core[m].at[q, j], w)]
                    if w == q - 1:
                        parts.append(cut(diag[m].at[q - 1, j], w))
                    total(cut(mine[m].at[q, j], w), *parts)
                remote(m, Q_X + 4 * (q - 1) + j, mine[m].at[q, j], side[m].at[q - 1, j], **to)

    def own(m):
        for j in (1, 2, 3, 0):
            pair(m, 0, j)
            arrived(m, Q_X + j, side[m].at[0, j])
            arrived(m, Q_X + 4 + j, side[m].at[1, j])
            total(mine[m].at[0, j], core[m].at[0, j], side[m].at[0, j], side[m].at[1, j])
            if j:
                remote(m, Q_O + j - 1, mine[m].at[0, j], line[m].at[j - 1], rz=j)

    def last(m):
        value = mine[m][0, 0].astype(F32)
        for j in range(3):
            arrived(m, Q_O + j, line[m].at[j])
            value = value + line[m][j].astype(F32)
        outs[m][...] = value

    stages = [corner, sides, own, last]
    for t in range(count + 3):
        for s in (3, 2, 1, 0):
            if 0 <= t - s < count:
                stages[s](t - s)
    for copy in started:
        copy.wait_send()


def scatter(arrays):
    count = len(arrays)
    shapes = [a.shape[-2:] for a in arrays]

    return pl.pallas_call(
        functools.partial(scatter_kernel, count),
        name="scatter",
        out_shape=tuple(jax.ShapeDtypeStruct(s, F32) for s in shapes),
        in_specs=[ANY] * count,
        out_specs=(pl.BlockSpec(memory_space=pltpu.VMEM),) * count,
        scratch_shapes=[pltpu.VMEM((4, 4) + s, BF16) for s in shapes]
        + [pltpu.VMEM((4, 4) + s, BF16) for s in shapes]
        + [pltpu.VMEM((2, 4) + s, BF16) for s in shapes]
        + [pltpu.VMEM((2, 4) + s, BF16) for s in shapes]
        + [pltpu.VMEM((3,) + s, BF16) for s in shapes]
        + [
            pltpu.SemaphoreType.DMA((count, Q_K)),
            pltpu.SemaphoreType.DMA((count, Q_K)),
            pltpu.SemaphoreType.DMA((count, 16)),
        ],
        compiler_params=pltpu.CompilerParams(collective_id=1, has_side_effects=True, vmem_limit_bytes=60 << 20),
    )(*arrays)


WIDTH = 768
HEADS = 12
HEAD_DIM = 64
LEN = 288


EPSILON = 1e-06
NEGATIVE = -1000000000.0
HALF_ROOT = 0.7071067811865476


def layer_norm(values, scales, shifts):
    centre = jnp.mean(values, axis=-1, keepdims=True)
    centred = values - centre
    spread = jnp.mean(centred * centred, axis=-1, keepdims=True)
    return centred * lax.rsqrt(spread + EPSILON) * scales + shifts


def gelu_exact(values):
    return 0.5 * values * (1.0 + lax.erf(values * HALF_ROOT))


def visible(segments, positions):
    offsets = positions - jnp.arange(positions.shape[-1], dtype=jnp.int32)[None, :]
    same_segment = segments[:, :, None] == segments[:, None, :]
    same_run = offsets[:, :, None] == offsets[:, None, :]
    return jnp.logical_and(same_segment, same_run)[:, None]


def project(left_side, right_side):
    return jnp.dot(left_side, right_side, preferred_element_type=jnp.float32)


def split_heads(tensor):
    return tensor.reshape(tensor.shape[0] // LEN, LEN, HEADS, HEAD_DIM)


def scaled_scores(query_heads, key_heads, allowed):
    raw_scores = jnp.einsum(
        "sqhd,skhd->shqk", query_heads, key_heads, preferred_element_type=jnp.float32
    )
    return jnp.where(allowed, raw_scores * 0.125, NEGATIVE)


def column_sums(gradient_low):
    return jnp.sum(gradient_low.astype(jnp.float32), axis=0)


def forward_pass(tokens, allowed, params):
    (
        query_weight,
        key_weight,
        value_weight,
        out_weight,
        up_weight,
        down_weight,
        query_bias,
        value_bias,
        out_bias,
        up_bias,
        down_bias,
        first_gain,
        first_shift,
        second_gain,
        second_shift,
    ) = params
    query_vectors = (project(tokens, query_weight) + query_bias).astype(jnp.bfloat16)
    key_vectors = project(tokens, key_weight).astype(jnp.bfloat16)
    value_vectors = (project(tokens, value_weight) + value_bias).astype(jnp.bfloat16)
    scores = scaled_scores(split_heads(query_vectors), split_heads(key_vectors), allowed)
    peak_score = jnp.max(scores, axis=-1, keepdims=True)
    exponents = jnp.exp(scores - peak_score)
    totals = jnp.sum(exponents, axis=-1, keepdims=True)
    probs_low = (exponents / totals).astype(jnp.bfloat16)
    log_total = peak_score + jnp.log(totals)
    attended = jnp.einsum(
        "shqk,skhd->sqhd", probs_low, split_heads(value_vectors), preferred_element_type=jnp.float32
    )
    mixed_heads = attended.reshape(tokens.shape).astype(jnp.bfloat16)
    first_in = tokens.astype(jnp.float32) + (project(mixed_heads, out_weight) + out_bias)
    first_out = layer_norm(first_in, first_gain, first_shift)
    first_low = first_out.astype(jnp.bfloat16)
    hidden = project(first_low, up_weight) + up_bias
    activated = gelu_exact(hidden).astype(jnp.bfloat16)
    second_in = first_out + (project(activated, down_weight) + down_bias)
    result = layer_norm(second_in, second_gain, second_shift).astype(jnp.bfloat16)
    saved_state = (
        query_vectors,
        key_vectors,
        value_vectors,
        log_total,
        mixed_heads,
        first_in,
        first_low,
        hidden,
        activated,
        second_in,
    )
    return (result, saved_state)


def ffn_backward(params, saved_state, cotangent):
    up_weight, down_weight = (params[4], params[5])
    second_gain, second_shift = (params[13], params[14])
    first_low, hidden, activated, second_in = (
        saved_state[6],
        saved_state[7],
        saved_state[8],
        saved_state[9],
    )
    unused, second_pull = jax.vjp(layer_norm, second_in, second_gain, second_shift)
    grad_second, second_gain_grad, second_shift_grad = second_pull(cotangent.astype(jnp.float32))
    output_low = grad_second.astype(jnp.bfloat16)
    down_weight_grad = jnp.einsum(
        "rf,rd->fd", activated, output_low, preferred_element_type=jnp.float32
    )
    down_bias_grad = column_sums(output_low)
    grad_activated = jnp.einsum(
        "rd,fd->rf", output_low, down_weight, preferred_element_type=jnp.float32
    )
    unused, gelu_pull = jax.vjp(gelu_exact, hidden)
    hidden_low = gelu_pull(grad_activated)[0].astype(jnp.bfloat16)
    up_weight_grad = jnp.einsum(
        "rd,rf->df", first_low, hidden_low, preferred_element_type=jnp.float32
    )
    up_bias_grad = column_sums(hidden_low)
    grad_first = grad_second + jnp.einsum(
        "rf,df->rd", hidden_low, up_weight, preferred_element_type=jnp.float32
    )
    return (
        grad_first,
        (
            up_weight_grad,
            down_weight_grad,
            up_bias_grad,
            down_bias_grad,
            second_gain_grad,
            second_shift_grad,
        ),
    )


def attention_backward(tokens, allowed, params, saved_state, grad_first):
    query_weight, key_weight, value_weight, out_weight = (
        params[0],
        params[1],
        params[2],
        params[3],
    )
    first_gain, first_shift = (params[11], params[12])
    query_vectors, key_vectors, value_vectors, log_total, mixed_heads, first_in = saved_state[:6]
    unused, first_pull = jax.vjp(layer_norm, first_in, first_gain, first_shift)
    grad_first_in, first_gain_grad, first_shift_grad = first_pull(grad_first)
    branch_low = grad_first_in.astype(jnp.bfloat16)
    out_weight_grad = jnp.einsum(
        "rd,re->de", mixed_heads, branch_low, preferred_element_type=jnp.float32
    )
    out_bias_grad = column_sums(branch_low)
    grad_mixed = split_heads(
        jnp.einsum("re,de->rd", branch_low, out_weight, preferred_element_type=jnp.float32).astype(
            jnp.bfloat16
        )
    )
    query_heads = split_heads(query_vectors)
    key_heads = split_heads(key_vectors)
    value_heads = split_heads(value_vectors)
    attention_probs = jnp.exp(scaled_scores(query_heads, key_heads, allowed) - log_total)
    values_grad = (
        jnp.einsum(
            "shqk,sqhd->skhd",
            attention_probs.astype(jnp.bfloat16),
            grad_mixed,
            preferred_element_type=jnp.float32,
        )
        .reshape(tokens.shape)
        .astype(jnp.bfloat16)
    )
    grad_probs = jnp.einsum(
        "sqhd,skhd->shqk", grad_mixed, value_heads, preferred_element_type=jnp.float32
    )
    centred_grad = grad_probs - jnp.sum(attention_probs * grad_probs, axis=-1, keepdims=True)
    scores_grad = (attention_probs * centred_grad).astype(jnp.bfloat16)
    queries_grad = (
        (
            0.125
            * jnp.einsum(
                "shqk,skhd->sqhd", scores_grad, key_heads, preferred_element_type=jnp.float32
            )
        )
        .reshape(tokens.shape)
        .astype(jnp.bfloat16)
    )
    keys_grad = (
        (
            0.125
            * jnp.einsum(
                "shqk,sqhd->skhd", scores_grad, query_heads, preferred_element_type=jnp.float32
            )
        )
        .reshape(tokens.shape)
        .astype(jnp.bfloat16)
    )
    query_weight_grad = jnp.einsum(
        "rd,re->de", tokens, queries_grad, preferred_element_type=jnp.float32
    )
    key_weight_grad = jnp.einsum("rd,re->de", tokens, keys_grad, preferred_element_type=jnp.float32)
    value_weight_grad = jnp.einsum(
        "rd,re->de", tokens, values_grad, preferred_element_type=jnp.float32
    )
    query_bias_grad = column_sums(queries_grad)
    value_bias_grad = column_sums(values_grad)
    token_grad = grad_first_in + jnp.einsum(
        "re,de->rd", queries_grad, query_weight, preferred_element_type=jnp.float32
    )
    token_grad = token_grad + jnp.einsum(
        "re,de->rd", keys_grad, key_weight, preferred_element_type=jnp.float32
    )
    token_grad = token_grad + jnp.einsum(
        "re,de->rd", values_grad, value_weight, preferred_element_type=jnp.float32
    )
    return (
        token_grad,
        (
            query_weight_grad,
            key_weight_grad,
            value_weight_grad,
            out_weight_grad,
            query_bias_grad,
            value_bias_grad,
            out_bias_grad,
            first_gain_grad,
            first_shift_grad,
        ),
    )


def pack_vectors(vectors, wide):
    rows = vectors[0].shape[0]
    columns = jnp.concatenate([jnp.stack(vectors, axis=1), wide.reshape(4, rows).T], axis=1)
    return jnp.pad(columns, ((0, 0), (0, 128 - columns.shape[1])))


def unpack_vectors(block, devices):
    rows = block.shape[0] // devices
    flat = block.T
    wide = flat[8:12].reshape(4, devices, rows).transpose(1, 0, 2).reshape(-1)
    return [flat[i] for i in range(8)], wide


def pack_sums(vectors, wide, devices):
    rows = vectors[0].shape[0] // devices
    flat = jnp.concatenate(
        [jnp.stack(vectors, axis=0), wide.reshape(devices, 4, rows).transpose(1, 0, 2).reshape(4, -1)],
        axis=0,
    )
    return jnp.pad(flat, ((0, 116), (0, 0))).T


def unpack_shard(block):
    return [block[:, i] for i in range(8)], block[:, 8:12].T.reshape(-1)


def gather_all(arrays, own):
    if own:
        return [g.reshape((-1, g.shape[-1])) for g in gather(arrays)]
    return [lax.all_gather(a, NAMES, axis=0, tiled=True) for a in arrays]


def scatter_all(arrays, devices, own):
    if own:
        return scatter([a.reshape((2, 2, 4, 2, a.shape[0] // devices, a.shape[1])) for a in arrays])
    return [
        lax.psum_scatter(a.astype(F32), NAMES, scatter_dimension=0, tiled=True) for a in arrays
    ]


def body(
    own, devices,
    tokens, segment_ids, position_ids, cotangent,
    query_weight, key_weight, value_weight, out_weight, up_weight, down_weight,
    query_bias, value_bias, out_bias, up_bias, down_bias,
    first_gain, first_shift, second_gain, second_shift,
):
    row_count = tokens.shape[0]
    allowed = visible(
        segment_ids.reshape(row_count // LEN, LEN), position_ids.reshape(row_count // LEN, LEN)
    )
    small = [query_bias, value_bias, out_bias, down_bias, first_gain, first_shift, second_gain, second_shift]
    packed = jnp.concatenate(
        [query_weight, key_weight, value_weight, out_weight, pack_vectors(small, up_bias)], axis=1
    )
    square, up, down = gather_all([packed, up_weight, down_weight], own)
    (qb, vb, ob, db, g1, s1, g2, s2), ub = unpack_vectors(square[:, 4 * WIDTH :].astype(F32), devices)
    params = tuple(square[:, i * WIDTH : (i + 1) * WIDTH] for i in range(4)) + (up, down)
    params = params + (qb, vb, ob, ub, db, g1, s1, g2, s2)
    result, saved_state = forward_pass(tokens, allowed, params)
    grad_first, ffn_grads = ffn_backward(params, saved_state, cotangent)
    dup, ddown, dub, ddb, dg2, ds2 = ffn_grads
    token_grad, attention_grads = attention_backward(
        tokens, allowed, params, saved_state, grad_first
    )
    dq, dk, dv, do, dqb, dvb, dob, dg1, ds1 = attention_grads
    sums = pack_sums([dqb, dvb, dob, ddb, dg1, ds1, dg2, ds2], dub, devices)
    dsquare = jnp.concatenate([t.astype(BF16) for t in (dq, dk, dv, do, sums)], axis=1)
    ddown, dup, dsquare = scatter_all(
        [ddown.astype(BF16), dup.astype(BF16), dsquare], devices, own
    )
    (dqb, dvb, dob, ddb, dg1, ds1, dg2, ds2), dub = unpack_shard(dsquare[:, 4 * WIDTH :])
    dq, dk, dv, do = (dsquare[:, i * WIDTH : (i + 1) * WIDTH] for i in range(4))
    return (
        result, token_grad, dq, dk, dv, do, dup, ddown,
        dqb, dvb, dob, dub, ddb, dg1, ds1, dg2, ds2,
    )


def solution(mesh):
    rows, flat = P(NAMES, None), P(NAMES)
    devices = mesh.shape["dp"] * mesh.shape["fsdp"]
    own = mesh.shape["dp"] == 4 and mesh.shape["fsdp"] == 8
    return jax.shard_map(
        functools.partial(body, own, devices),
        mesh=mesh,
        in_specs=(rows, flat, flat) + (rows,) * 7 + (flat,) * 9,
        out_specs=(rows,) * 8 + (flat,) * 9,
        check_vma=False,
    )
```

```python
import functools
import jax
import jax.numpy as jnp
from jax import lax
from jax.sharding import PartitionSpec as P
from jax.experimental import pallas as pl
from jax.experimental.pallas import tpu as pltpu

MESH = pl.DeviceIdType.MESH
ANY = pl.BlockSpec(memory_space=pl.ANY)
F32 = jnp.float32
BF16 = jnp.bfloat16


NAMES = ('dp', 'fsdp')


class Place:
    def __init__(self):
        dp, fs = lax.axis_index("dp"), lax.axis_index("fsdp")
        self.y, self.c = dp // 2, dp % 2
        self.z, self.x = fs // 2, fs % 2

    def device(self, ry=0, rc=0, rz=0, rx=0):
        y = 1 - self.y if ry else self.y
        c = 1 - self.c if rc else self.c
        x = 1 - self.x if rx else self.x
        return (y * 2 + c, ((self.z + rz) % 4) * 2 + x)

    def slot(self, ry=0, rc=0, rz=0, rx=0):
        y = 1 - self.y if ry else self.y
        c = 1 - self.c if rc else self.c
        x = 1 - self.x if rx else self.x
        return (y, c, (self.z + rz) % 4, x)


def greet(me):
    barrier = pltpu.get_barrier_semaphore()
    peers = [me.device(rx=1), me.device(ry=1), me.device(rc=1)]
    peers += [me.device(rz=k) for k in (1, 2, 3)]
    for peer in peers:
        pl.semaphore_signal(barrier, inc=1, device_id=peer, device_id_type=MESH)
    pl.semaphore_wait(barrier, 6)


def halves(ref, lead, which):
    r, n = ref.shape[-2:]
    if r >= 96:
        return ref.at[(*lead, pl.ds(which * (r // 2), r // 2), slice(None))]
    first = n // 256 * 128
    return ref.at[(*lead, slice(None), pl.ds(first if which else 0, n - first if which else first))]


Z, X, Y, XY, YX, C0, CX, CY, CB, CC, KINDS = 0, 3, 7, 11, 15, 19, 23, 27, 31, 35, 39


def gather_kernel(count, *refs):
    ins, outs = refs[:count], refs[count : 2 * count]
    bounce = refs[2 * count : 3 * count]
    send, recv, local = refs[3 * count :]
    me = Place()
    greet(me)
    started = []

    def remote(m, k, src, dst, **to):
        copy = pltpu.make_async_remote_copy(
            src_ref=src, dst_ref=dst, send_sem=send.at[m, k], recv_sem=recv.at[m, k],
            device_id=me.device(**to), device_id_type=MESH,
        )
        copy.start()
        started.append(copy)

    def arrived(m, k, dst):
        pltpu.make_async_remote_copy(
            src_ref=dst, dst_ref=dst, send_sem=send.at[m, k], recv_sem=recv.at[m, k],
            device_id=me.device(rc=1), device_id_type=MESH,
        ).wait_recv()

    for m in range(count):
        pltpu.make_async_copy(ins[m], bounce[m], local.at[m]).start()
    for m in range(count):
        for k in (1, 2, 3):
            remote(m, Z + k - 1, ins[m], outs[m].at[me.slot()], rz=k)
    for m in range(count):
        pltpu.make_async_copy(ins[m], bounce[m], local.at[m]).wait()
        pltpu.make_async_copy(bounce[m], outs[m].at[me.slot()], local.at[m]).start()

    def diagonal(m, j):
        slot = me.slot(rz=-j, rx=1, ry=1)
        b, c = halves(outs[m], slot, 0), halves(outs[m], slot, 1)
        arrived(m, XY + j, b)
        remote(m, CB + j, b, b, rc=1)
        arrived(m, YX + j, c)
        remote(m, CC + j, c, c, rc=1)

    def across(m, j):
        sx = me.slot(rz=-j, rx=1)
        arrived(m, X + j, outs[m].at[sx])
        b = halves(outs[m], sx, 0)
        remote(m, XY + j, b, b, ry=1)
        remote(m, CX + j, outs[m].at[sx], outs[m].at[sx], rc=1)
        sy = me.slot(rz=-j, ry=1)
        arrived(m, Y + j, outs[m].at[sy])
        c = halves(outs[m], sy, 1)
        remote(m, YX + j, c, c, rx=1)
        remote(m, CY + j, outs[m].at[sy], outs[m].at[sy], rc=1)

    def along(m, j):
        slot = me.slot(rz=-j)
        dst = outs[m].at[slot]
        src = ins[m] if j == 0 else dst
        if j:
            arrived(m, Z + j - 1, dst)
        remote(m, X + j, src, dst, rx=1)
        remote(m, Y + j, src, dst, ry=1)
        remote(m, C0 + j, src, dst, rc=1)

    for m in range(count):
        along(m, 0)
        for j in range(1, 4):
            along(m, j)
            across(m, j - 1)
        across(m, 3)
        for j in range(4):
            diagonal(m, j)
    for m in range(count):
        for j in range(4):
            arrived(m, C0 + j, outs[m].at[me.slot(rc=1, rz=-j)])
            arrived(m, CX + j, outs[m].at[me.slot(rc=1, rz=-j, rx=1)])
            arrived(m, CY + j, outs[m].at[me.slot(rc=1, rz=-j, ry=1)])
            slot = me.slot(rc=1, rz=-j, rx=1, ry=1)
            arrived(m, CB + j, halves(outs[m], slot, 0))
            arrived(m, CC + j, halves(outs[m], slot, 1))
    for copy in started:
        copy.wait_send()
    for m in range(count):
        pltpu.make_async_copy(bounce[m], outs[m].at[me.slot()], local.at[m]).wait()


def gather(arrays):
    count = len(arrays)
    return pl.pallas_call(
        functools.partial(gather_kernel, count),
        name="gather",
        out_shape=tuple(jax.ShapeDtypeStruct((2, 2, 4, 2) + a.shape, a.dtype) for a in arrays),
        in_specs=[ANY] * count,
        out_specs=(ANY,) * count,
        scratch_shapes=[pltpu.VMEM(a.shape, a.dtype) for a in arrays]
        + [
            pltpu.SemaphoreType.DMA((count, KINDS)),
            pltpu.SemaphoreType.DMA((count, KINDS)),
            pltpu.SemaphoreType.DMA((count,)),
        ],
        compiler_params=pltpu.CompilerParams(collective_id=0, has_side_effects=True),
    )(*arrays)


Q_C, Q_D, Q_X, Q_O, Q_K = 0, 16, 24, 32, 35


def scatter_kernel(count, *refs):
    ins, outs = refs[:count], refs[count : 2 * count]
    rest = refs[2 * count :]
    mine, core, diag, side, line = (rest[i * count : (i + 1) * count] for i in range(5))
    send, recv, local = rest[5 * count :]
    me = Place()
    greet(me)
    started = []

    def remote(m, k, src, dst, **to):
        copy = pltpu.make_async_remote_copy(
            src_ref=src, dst_ref=dst, send_sem=send.at[m, k], recv_sem=recv.at[m, k],
            device_id=me.device(**to), device_id_type=MESH,
        )
        copy.start()
        started.append(copy)

    def arrived(m, k, dst):
        pltpu.make_async_remote_copy(
            src_ref=dst, dst_ref=dst, send_sem=send.at[m, k], recv_sem=recv.at[m, k],
            device_id=me.device(rc=1), device_id_type=MESH,
        ).wait_recv()

    quarters = {3: dict(rx=1, ry=1), 1: dict(rx=1), 2: dict(ry=1), 0: {}}

    def load(m, q, j):
        slot = me.slot(rz=j, **quarters[q])
        return pltpu.make_async_copy(ins[m].at[slot], mine[m].at[q, j], local.at[m, q * 4 + j])

    for m in range(count):
        for q in (3, 1, 2, 0):
            for j in range(4):
                slot = me.slot(rz=j, rc=1, **quarters[q])
                remote(m, Q_C + q * 4 + j, ins[m].at[slot], core[m].at[q, j], rc=1)
                load(m, q, j).start()

    def cut(ref, which):
        return halves(ref, (), which)

    def pair(m, q, j):
        load(m, q, j).wait()
        arrived(m, Q_C + q * 4 + j, core[m].at[q, j])

    def total(dst, *parts):
        value = dst[...].astype(F32)
        for part in parts:
            value = value + part[...].astype(F32)
        dst[...] = value.astype(dst.dtype)

    def corner(m):
        for j in range(4):
            pair(m, 3, j)
            total(mine[m].at[3, j], core[m].at[3, j])
            remote(m, Q_D + j, cut(mine[m].at[3, j], 0), cut(diag[m].at[0, j], 0), ry=1)
            remote(m, Q_D + 4 + j, cut(mine[m].at[3, j], 1), cut(diag[m].at[1, j], 1), rx=1)

    def sides(m):
        for j in range(4):
            for q, to in ((1, dict(rx=1)), (2, dict(ry=1))):
                pair(m, q, j)
                arrived(m, Q_D + 4 * (q - 1) + j, cut(diag[m].at[q - 1, j], q - 1))
                for w in (0, 1):
                    parts = [cut(core[m].at[q, j], w)]
                    if w == q - 1:
                        parts.append(cut(diag[m].at[q - 1, j], w))
                    total(cut(mine[m].at[q, j], w), *parts)
                remote(m, Q_X + 4 * (q - 1) + j, mine[m].at[q, j], side[m].at[q - 1, j], **to)

    def own(m):
        for j in (1, 2, 3, 0):
            pair(m, 0, j)
            arrived(m, Q_X + j, side[m].at[0, j])
            arrived(m, Q_X + 4 + j, side[m].at[1, j])
            total(mine[m].at[0, j], core[m].at[0, j], side[m].at[0, j], side[m].at[1, j])
            if j:
                remote(m, Q_O + j - 1, mine[m].at[0, j], line[m].at[j - 1], rz=j)

    def last(m):
        value = mine[m][0, 0].astype(F32)
        for j in range(3):
            arrived(m, Q_O + j, line[m].at[j])
            value = value + line[m][j].astype(F32)
        outs[m][...] = value

    stages = [corner, sides, own, last]
    for t in range(count + 3):
        for s in (3, 2, 1, 0):
            if 0 <= t - s < count:
                stages[s](t - s)
    for copy in started:
        copy.wait_send()


def scatter(arrays):
    count = len(arrays)
    shapes = [a.shape[-2:] for a in arrays]

    return pl.pallas_call(
        functools.partial(scatter_kernel, count),
        name="scatter",
        out_shape=tuple(jax.ShapeDtypeStruct(s, F32) for s in shapes),
        in_specs=[ANY] * count,
        out_specs=(pl.BlockSpec(memory_space=pltpu.VMEM),) * count,
        scratch_shapes=[pltpu.VMEM((4, 4) + s, BF16) for s in shapes]
        + [pltpu.VMEM((4, 4) + s, BF16) for s in shapes]
        + [pltpu.VMEM((2, 4) + s, BF16) for s in shapes]
        + [pltpu.VMEM((2, 4) + s, BF16) for s in shapes]
        + [pltpu.VMEM((3,) + s, BF16) for s in shapes]
        + [
            pltpu.SemaphoreType.DMA((count, Q_K)),
            pltpu.SemaphoreType.DMA((count, Q_K)),
            pltpu.SemaphoreType.DMA((count, 16)),
        ],
        compiler_params=pltpu.CompilerParams(collective_id=1, has_side_effects=True, vmem_limit_bytes=60 << 20),
    )(*arrays)


HEADS = 12
HEAD_DIM = 64
LEN = 288
WIDTH = 768
EPSILON = 1e-06
NEGATIVE = -1000000000.0
HALF_ROOT = 0.7071067811865476
LANES = 256
GROUPS = WIDTH // LANES
PER = LANES // HEAD_DIM


def nn(a, b):
    return lax.dot_general(a, b, (((1,), (0,)), ((), ())), preferred_element_type=F32)


def nt(a, b):
    return lax.dot_general(a, b, (((1,), (1,)), ((), ())), preferred_element_type=F32)


def tn(a, b):
    return lax.dot_general(a, b, (((0,), (0,)), ((), ())), preferred_element_type=F32)


def keep(block, head):
    lane = lax.broadcasted_iota(jnp.int32, block.shape, 1)
    mine = lane < HEAD_DIM if head == 0 else lane >= HEAD_DIM
    return jnp.where(mine, block, jnp.zeros_like(block))


def attend_kernel(column, row, q_ref, k_ref, v_ref, mixed, probs):
    allowed = column[...] == row[0]
    for pair in range(LANES // 128):
        lanes = pl.ds(pair * 128, 128)
        q2, k2, v2 = q_ref[:, lanes], k_ref[:, lanes], v_ref[:, lanes]
        out = None
        for head in (0, 1):
            scores = jnp.where(allowed, nt(k2, keep(q2, head)) * 0.125, NEGATIVE)
            peak = jnp.max(scores, axis=0, keepdims=True)
            powers = jnp.exp(scores - peak)
            low = (powers * (1.0 / jnp.sum(powers, axis=0, keepdims=True))).astype(BF16)
            probs[0, 2 * pair + head] = low
            part = tn(low, keep(v2, head))
            out = part if out is None else out + part
        mixed[:, lanes] = out.astype(BF16)


def attend(qkv, code):
    rows = qkv.shape[0]
    seqs = rows // LEN
    block = lambda part: pl.BlockSpec((LEN, LANES), lambda s, g: (s, part * GROUPS + g))
    return pl.pallas_call(
        attend_kernel,
        name="attend",
        grid=(seqs, GROUPS),
        out_shape=(
            jax.ShapeDtypeStruct((rows, WIDTH), BF16),
            jax.ShapeDtypeStruct((seqs, HEADS, LEN, LEN), BF16),
        ),
        in_specs=[
            pl.BlockSpec((LEN, 1), lambda s, g: (s, 0)),
            pl.BlockSpec((1, 1, LEN), lambda s, g: (s, 0, 0)),
            block(0), block(1), block(2),
        ],
        out_specs=(
            pl.BlockSpec((LEN, LANES), lambda s, g: (s, g)),
            pl.BlockSpec((1, PER, LEN, LEN), lambda s, g: (s, g, 0, 0)),
        ),
    )(code.reshape(rows, 1), code.reshape(seqs, 1, LEN), qkv, qkv, qkv)


def attend_back_kernel(q_ref, k_ref, v_ref, g_ref, probs, out):
    base = pl.program_id(1) * LANES
    for pair in range(LANES // 128):
        lanes = pl.ds(pair * 128, 128)
        q2, k2, v2, g2 = q_ref[:, lanes], k_ref[:, lanes], v_ref[:, lanes], g_ref[:, lanes]
        dq = dk = dv = 0.0
        for head in (0, 1):
            low = probs[0, 2 * pair + head]
            wide = low.astype(F32)
            gh = keep(g2, head)
            gp = nt(v2, gh)
            centre = jnp.sum(wide * gp, axis=0, keepdims=True)
            ds = (wide * (gp - centre)).astype(BF16)
            dv = dv + nn(low, gh)
            dk = dk + nn(ds, keep(q2, head))
            dq = dq + tn(ds, keep(k2, head))
        for part, value in enumerate((0.125 * dq, 0.125 * dk, dv)):
            at = pl.multiple_of(base + (part * WIDTH + pair * 128), 128)
            out[:, pl.ds(at, 128)] = value.astype(BF16)


def attend_back(qkv, grad, probs):
    rows = qkv.shape[0]
    seqs = rows // LEN
    block = lambda part: pl.BlockSpec((LEN, LANES), lambda s, g: (s, part * GROUPS + g))
    return pl.pallas_call(
        attend_back_kernel,
        name="attend_back",
        grid=(seqs, GROUPS),
        out_shape=jax.ShapeDtypeStruct((rows, 3 * WIDTH), BF16),
        in_specs=[
            block(0), block(1), block(2), block(0),
            pl.BlockSpec((1, PER, LEN, LEN), lambda s, g: (s, g, 0, 0)),
        ],
        out_specs=pl.BlockSpec((LEN, 3 * WIDTH), lambda s, g: (s, 0)),
    )(qkv, qkv, qkv, grad, probs)


def layer_norm(values, scales, shifts):
    centre = jnp.mean(values, axis=-1, keepdims=True)
    centred = values - centre
    spread = jnp.mean(centred * centred, axis=-1, keepdims=True)
    return centred * lax.rsqrt(spread + EPSILON) * scales + shifts


def gelu_exact(values):
    return 0.5 * values * (1.0 + lax.erf(values * HALF_ROOT))


def column_sums(gradient_low):
    return jnp.sum(gradient_low.astype(F32), axis=0)


def run_codes(segments, positions):
    run = positions - jnp.arange(segments.shape[0], dtype=jnp.int32) % LEN
    return segments * 1024 + run


def layer(tokens, codes, cotangent, square, up, down, vectors, wide):
    qb, vb, ob, db, g1, s1, g2, s2 = vectors
    qkv_weight, out_weight = square[:, : 3 * WIDTH], square[:, 3 * WIDTH : 4 * WIDTH]
    bias = jnp.concatenate([qb, jnp.zeros_like(qb), vb])
    qkv = (nn(tokens, qkv_weight) + bias).astype(BF16)
    mixed, probs = attend(qkv, codes)
    first_in = tokens.astype(F32) + (nn(mixed, out_weight) + ob)
    first, first_pull = jax.vjp(layer_norm, first_in, g1, s1)
    first_low = first.astype(BF16)
    hidden = nn(first_low, up) + wide
    activated, gelu_pull = jax.vjp(gelu_exact, hidden)
    activated = activated.astype(BF16)
    second_in = first + (nn(activated, down) + db)
    result, second_pull = jax.vjp(layer_norm, second_in, g2, s2)

    grad_second, dg2, ds2 = second_pull(cotangent.astype(F32))
    output_low = grad_second.astype(BF16)
    ddown = tn(activated, output_low).astype(BF16)
    ddb = column_sums(output_low)
    hidden_low = gelu_pull(nt(output_low, down))[0].astype(BF16)
    dup = tn(first_low, hidden_low).astype(BF16)
    dwide = column_sums(hidden_low)
    grad_first = grad_second + nt(hidden_low, up)
    grad_first_in, dg1, ds1 = first_pull(grad_first)
    branch_low = grad_first_in.astype(BF16)
    dout = tn(mixed, branch_low).astype(BF16)
    dob = column_sums(branch_low)
    grad_mixed = nt(branch_low, out_weight).astype(BF16)
    dqkv = attend_back(qkv, grad_mixed, probs)
    dqkv_weight = tn(tokens, dqkv).astype(BF16)
    dbias = column_sums(dqkv)
    token_grad = grad_first_in + nt(dqkv, qkv_weight)
    sums = [dbias[:WIDTH], dbias[2 * WIDTH :], dob, ddb, dg1, ds1, dg2, ds2]
    return result.astype(BF16), token_grad, ddown, dup, dout, dqkv_weight, sums, dwide


def pack_vectors(vectors, wide):
    rows = vectors[0].shape[0]
    columns = jnp.concatenate([jnp.stack(vectors, axis=1), wide.reshape(4, rows).T], axis=1)
    return jnp.pad(columns, ((0, 0), (0, 128 - columns.shape[1])))


def unpack_vectors(block, devices):
    rows = block.shape[0] // devices
    flat = block.T
    wide = flat[8:12].reshape(4, devices, rows).transpose(1, 0, 2).reshape(-1)
    return [flat[i] for i in range(8)], wide


def pack_sums(vectors, wide, devices):
    rows = vectors[0].shape[0] // devices
    flat = jnp.concatenate(
        [jnp.stack(vectors, axis=0), wide.reshape(devices, 4, rows).transpose(1, 0, 2).reshape(4, -1)],
        axis=0,
    )
    return jnp.pad(flat, ((0, 116), (0, 0))).T


def unpack_shard(block):
    return [block[:, i] for i in range(8)], block[:, 8:12].T.reshape(-1)


def gather_all(arrays, own):
    if own:
        return [g.reshape((-1, g.shape[-1])) for g in gather(arrays)]
    return [lax.all_gather(a, NAMES, axis=0, tiled=True) for a in arrays]


def scatter_all(arrays, devices, own):
    if own:
        return scatter([a.reshape((2, 2, 4, 2, a.shape[0] // devices, a.shape[1])) for a in arrays])
    return [
        lax.psum_scatter(a.astype(F32), NAMES, scatter_dimension=0, tiled=True) for a in arrays
    ]


def body(
    own, devices,
    tokens, segment_ids, position_ids, cotangent,
    query_weight, key_weight, value_weight, out_weight, up_weight, down_weight,
    query_bias, value_bias, out_bias, up_bias, down_bias,
    first_gain, first_shift, second_gain, second_shift,
):
    small = [query_bias, value_bias, out_bias, down_bias, first_gain, first_shift, second_gain, second_shift]
    packed = jnp.concatenate(
        [query_weight, key_weight, value_weight, out_weight, pack_vectors(small, up_bias)], axis=1
    )
    square, up, down = gather_all([packed, up_weight, down_weight], own)
    vectors, wide = unpack_vectors(square[:, 4 * WIDTH :].astype(F32), devices)
    codes = run_codes(segment_ids, position_ids)
    result, token_grad, ddown, dup, dout, dqkv, sums, dwide = layer(
        tokens, codes, cotangent, square, up, down, vectors, wide
    )
    sums = pack_sums(sums, dwide, devices).astype(BF16)
    dout = jnp.concatenate([dout, sums], axis=1)
    ddown, dup, dout, dqkv = scatter_all([ddown, dup, dout, dqkv], devices, own)
    (dqb, dvb, dob, ddb, dg1, ds1, dg2, ds2), dub = unpack_shard(dout[:, WIDTH:])
    dq, dk, dv = (dqkv[:, i * WIDTH : (i + 1) * WIDTH] for i in range(3))
    return (
        result, token_grad, dq, dk, dv, dout[:, :WIDTH], dup, ddown,
        dqb, dvb, dob, dub, ddb, dg1, ds1, dg2, ds2,
    )


def solution(mesh):
    rows, flat = P(NAMES, None), P(NAMES)
    devices = mesh.shape["dp"] * mesh.shape["fsdp"]
    own = mesh.shape["dp"] == 4 and mesh.shape["fsdp"] == 8
    return jax.shard_map(
        functools.partial(body, own, devices),
        mesh=mesh,
        in_specs=(rows, flat, flat) + (rows,) * 7 + (flat,) * 9,
        out_specs=(rows,) * 8 + (flat,) * 9,
        check_vma=False,
    )
```
